32 devices in a mesh: member: 4 (over y, core), space: 8 (over z, x).
Axes of the slice: x: 2, y: 2, z: 4, core: 2. Of those that a mesh axis runs over, the one named last changes fastest.
Arguments:
- state: float32 [256, 128, 1024], P('member', 'space'), may hold values from -8 to 8
- obs_index: int32 [8192], P('space'), may hold values from 0 to 16383
- obs_value: float32 [8192], P('space'), may hold values from -6 to 6
- obs_scale: float32 [8192], P('space'), may hold values from 0.3 to 3
- ksat: float32 [128, 1024], P('space'), may hold values from 0.05 to 0.2
- storage: float32 [128, 1024], P('space'), may hold values from 0.5 to 4
- recharge: float32 [128, 1024], P('space'), may hold values from -1.8 to 1.8
- newton_counts: int32 [256], replicated, may hold values from 1 to 8, as said below
Outputs:
- forecast: float32 [256, 128, 1024], P('member', 'space')
The draws below stay inside these ranges and needn't reach their ends.
Inputs may be any that keep to these rules, and one draw needn't show every extreme that they name: `newton_counts`: A count of 8 occurs in every draw.
All inputs are finite; a program needn't handle non-finite values.
Results may differ from the reference program's by a relative error of at most 0.0003.
Values sent between devices are 32-bit elements; how exact they have to be, the bound alone decides.
A program may use at most 64 MiB of HBM per device.

```python
import math
import jax
import jax.numpy as jnp
from jax import lax

M = 256
CX = 16
NY = 1024
NOBS_DEV = 1024
KMAX = 8
NS_ITERS = 12
NX = 128
NOBS = 8192


def draw_state(key, part):
    key_one, key_two, key_three = jax.random.split(jax.random.fold_in(key, 11), 3)
    member_scale = jnp.exp(jax.random.uniform(key_one, (M, 1, 1), jnp.float32, math.log(0.1), 0.0))
    noise = jnp.clip(jax.random.normal(key_two, (M, NX, NY), jnp.float32), -4.0, 4.0)
    centre = jnp.clip(jax.random.normal(key_three, (1, NX, NY), jnp.float32), -4.0, 4.0)
    return (centre + member_scale * noise).astype(jnp.float32)


def draw_recharge(key, part):
    key_one, key_two = jax.random.split(jax.random.fold_in(key, 37))
    phases = jax.random.uniform(key_one, (4,), jnp.float32, 0.0, 2.0 * math.pi)
    row_place = (jnp.arange(NX, dtype=jnp.float32) / NX)[:, None]
    col_place = (jnp.arange(NY, dtype=jnp.float32) / NY)[None, :]
    waves = jnp.sin(2.0 * math.pi * 3.0 * row_place + phases[0]) * jnp.cos(2.0 * math.pi * 2.0 * col_place + phases[1])
    bent = waves + 0.3 * jnp.sin(2.0 * math.pi * 5.0 * col_place + phases[2]) * jnp.cos(2.0 * math.pi * 4.0 * row_place + phases[3])
    smooth = jnp.tanh(3.0 * bent)
    rough = 0.5 * jnp.clip(jax.random.normal(key_two, (NX, NY), jnp.float32), -2.0, 2.0)
    value = 0.7 * smooth + 0.3 * rough
    return (1.8 * jnp.clip(value, -1.0, 1.0)).astype(jnp.float32)


def draw_newton_counts(key, part):
    key_one, key_two = jax.random.split(jax.random.fold_in(key, 23))
    low_counts = jax.random.randint(key_one, (M,), 1, 4, dtype=jnp.int32)
    run_start = jax.random.randint(key_two, (), 0, M, dtype=jnp.int32)
    distance = (jnp.arange(M, dtype=jnp.int32) - run_start) % M
    return jnp.where(distance < M // 8, KMAX, low_counts).astype(jnp.int32)


def place_ends(drawn, key, low, top_value):
    dims = drawn.shape
    index_at = [jax.random.randint(jax.random.fold_in(key, axis), (), 0, dims[axis]) for axis in range(len(dims))]
    drawn = drawn.at[tuple(index_at)].set(low)
    longest = dims.index(max(dims))
    index_at[longest] = (index_at[longest] + 1) % dims[longest]
    return drawn.at[tuple(index_at)].set(top_value)


def block_scale(key, dims, shards, least, high):
    loudness, own = 1.0, jax.random.fold_in(key, 6)
    for position, parts in shards:
        heights = jnp.exp(jax.random.uniform(jax.random.fold_in(own, position), (parts,), jnp.float32, least / len(shards), high / len(shards)))
        loudness = loudness * jnp.repeat(heights, dims[position] // parts).reshape([-1 if axis == position else 1 for axis in range(len(dims))])
    return loudness


def centred(stream_key, dims, scale, bound, cuts=(), kind=jnp.bfloat16):
    values = jax.random.normal(stream_key, dims, jnp.float32) * scale
    if len(cuts) > 0:
        values = block_scale(stream_key, dims, cuts, -0.22, 0.18) * values
    return jnp.clip(values, min=-bound, max=bound).astype(kind)


def setup_inputs(seed: int = 0) -> dict:
    keys = jax.random.split(jax.random.key(seed), 9)
    state = draw_state(jax.random.fold_in(keys[8], 71), 0)
    obs_index = place_ends(jax.random.randint(keys[1], (NOBS,), 0, CX * NY), jax.random.fold_in(keys[1], 1), 0, (CX * NY) - 1).astype(jnp.int32)
    obs_value = centred(keys[2], (NOBS,), 1.0, 6.0, ((0, 8),), jnp.float32)
    obs_scale = jnp.clip(jnp.exp(math.log(3.0) - 2.3025851 * jax.random.uniform(keys[3], (NOBS,), jnp.float32) ** block_scale(keys[3], (NOBS,), ((0, 8),), -0.2, 0.2)), 0.3, 3.0)
    ksat = jnp.clip(jnp.exp(math.log(0.2) - 1.3862944 * jax.random.uniform(keys[4], (NX, NY), jnp.float32) ** block_scale(keys[4], (NX, NY), ((0, 8),), -0.2, 0.2)), 0.05, 0.2)
    storage = jnp.clip(jnp.exp(math.log(4.0) - 2.0794415 * jax.random.uniform(keys[5], (NX, NY), jnp.float32) ** block_scale(keys[5], (NX, NY), ((0, 8),), -0.2, 0.2)), 0.5, 4.0)
    recharge = draw_recharge(jax.random.fold_in(keys[8], 71), 0)
    newton_counts = draw_newton_counts(jax.random.fold_in(keys[8], 71), 0)
    return dict(state=state, obs_index=obs_index, obs_value=obs_value, obs_scale=obs_scale, ksat=ksat, storage=storage, recharge=recharge, newton_counts=newton_counts)


HIGHEST_PRECISION = lax.Precision.HIGHEST
DAMPING = 0.3

def inverse_root(gram_matrix):
    order_size = gram_matrix.shape[0]
    identity = jnp.eye(order_size, dtype=jnp.float32)
    whole = identity + gram_matrix
    norm_value = jnp.sqrt(jnp.sum(whole * whole))
    upper_iter = whole / norm_value
    lower_iter = identity
    for sweep_index in range(NS_ITERS):
        middle = 1.5 * identity - 0.5 * jnp.dot(lower_iter, upper_iter, precision=HIGHEST_PRECISION)
        upper_iter = jnp.dot(upper_iter, middle, precision=HIGHEST_PRECISION)
        lower_iter = jnp.dot(middle, lower_iter, precision=HIGHEST_PRECISION)
    return lower_iter / jnp.sqrt(norm_value)

def face_flux(padded, conduct):
    wide_level = jnp.pad(padded, ((0, 0), (0, 0), (1, 1)))
    wide_cond = jnp.pad(conduct, ((0, 0), (0, 0), (1, 1)))
    centre_level = wide_level[:, 1:-1, 1:-1]
    centre_cond = wide_cond[:, 1:-1, 1:-1]
    height = centre_level.shape[1]
    breadth = centre_level.shape[2]
    divergence = jnp.zeros_like(centre_level)
    for offset_row, offset_col in ((0, 1), (2, 1), (1, 0), (1, 2)):
        other_level = wide_level[:, offset_row:offset_row + height, offset_col:offset_col + breadth]
        other_cond = wide_cond[:, offset_row:offset_row + height, offset_col:offset_col + breadth]
        divergence = divergence + 0.5 * (centre_cond + other_cond) * (other_level - centre_level)
    return divergence

def relax(pressure, drive_term, storage, counts):
    target = pressure + storage * jnp.tanh(pressure) + drive_term
    iterate = pressure
    for sweep_index in range(KMAX):
        bend_value = jnp.tanh(iterate)
        derivative = 1.0 + storage * (1.0 - bend_value * bend_value)
        stepped = iterate - DAMPING * (iterate + storage * bend_value - target) / derivative
        iterate = jnp.where((counts > sweep_index)[:, None, None], stepped, iterate)
    return iterate

def advance(pressure, ksat, storage, recharge, counts):
    padded = jnp.pad(pressure, ((0, 0), (1, 1), (0, 0)))
    padded_ksat = jnp.pad(ksat, ((1, 1), (0, 0)))
    conduct = padded_ksat * jax.nn.sigmoid(padded)
    drive_term = face_flux(padded, conduct) + recharge
    return relax(pressure, drive_term, storage, counts)

def reference(state, obs_index, obs_value, obs_scale, ksat, storage, recharge, newton_counts):
    members = state.shape[0]
    flattened = state.reshape(members, NX * NY)
    mean_state = lax.optimization_barrier(jnp.mean(flattened, axis=0))
    anomaly = flattened - mean_state
    tile_of = jnp.arange(obs_index.shape[0], dtype=jnp.int32) // NOBS_DEV
    observed = (tile_of * (CX * NY) + obs_index).astype(jnp.int32)
    root_count = jnp.sqrt(jnp.float32(members - 1))
    spread = jnp.take(anomaly, observed, axis=1) * obs_scale / root_count
    innovation = obs_scale * (obs_value - jnp.take(mean_state, observed))
    gram_matrix = jnp.dot(spread, spread.T, precision=HIGHEST_PRECISION)
    drive_vector = jnp.dot(spread, innovation, precision=HIGHEST_PRECISION)
    root_inverse = inverse_root(gram_matrix)
    mean_weights = jnp.dot(root_inverse, jnp.dot(root_inverse, drive_vector, precision=HIGHEST_PRECISION), precision=HIGHEST_PRECISION)
    transform = mean_weights[:, None] / root_count + root_inverse

    def one_group(inputs):
        columns, counts = inputs
        analysis = mean_state + jnp.dot(columns.T, anomaly, precision=HIGHEST_PRECISION)
        pressure = analysis.reshape(columns.shape[1], NX, NY)
        for step_index in range(2):
            pressure = advance(pressure, ksat, storage, recharge, counts)
        return pressure
    grouped = transform.reshape(members, members // 8, 8).transpose(1, 0, 2)
    counts_grouped = newton_counts.reshape(members // 8, 8)
    result = lax.map(one_group, (grouped, counts_grouped))
    return result.reshape(members, NX, NY)
```

```python
import functools

import jax
import jax.numpy as jnp
from jax import lax
from jax.experimental import pallas as pl
from jax.experimental.pallas import tpu as pltpu
from jax.sharding import PartitionSpec as P


NS_ITERS = 12
HIGHEST_PRECISION = lax.Precision.HIGHEST
DAMPING = 0.3
GROUP = 8


def inverse_root(gram_matrix):
    order_size = gram_matrix.shape[0]
    identity = jnp.eye(order_size, dtype=jnp.float32)
    whole = identity + gram_matrix
    norm_value = jnp.sqrt(jnp.sum(whole * whole))
    upper_iter = whole / norm_value
    lower_iter = identity
    for _ in range(NS_ITERS):
        middle = 1.5 * identity - 0.5 * jnp.dot(lower_iter, upper_iter, precision=HIGHEST_PRECISION)
        upper_iter = jnp.dot(upper_iter, middle, precision=HIGHEST_PRECISION)
        lower_iter = jnp.dot(middle, lower_iter, precision=HIGHEST_PRECISION)
    return lower_iter / jnp.sqrt(norm_value)


def halves(value):
    high = value.astype(jnp.bfloat16)
    low = (value - high.astype(jnp.float32)).astype(jnp.bfloat16)
    return high, low


def analysis_kernel(rows, count, *refs):
    weight_high, weight_low = halves(refs[0][...])
    pieces = refs[1 : 1 + count]
    out_ref, first_ref, last_ref = refs[1 + count :]
    own = weight_high.shape[0]
    both = jnp.concatenate([weight_high, weight_low], axis=0)
    for row in range(0, rows, 2):
        columns = []
        for line in (row, row + 1):
            stacked = [piece[pl.ds(line, piece.shape[0] // rows, stride=rows), :] for piece in pieces]
            columns.append(jnp.concatenate(stacked, axis=0))
        high, low = halves(jnp.concatenate(columns, axis=1))
        wide = jnp.dot(both, high, preferred_element_type=jnp.float32)
        result = wide[:own] + wide[own:]
        result = result + jnp.dot(weight_high, low, preferred_element_type=jnp.float32)
        lanes = out_ref.shape[1]
        for index, line in enumerate((row, row + 1)):
            out_ref[pl.ds(line, own, stride=rows), :] = result[:, index * lanes : (index + 1) * lanes]
        if row == 0:
            first_ref[...] = result[:, :lanes]
        if row == rows - 2:
            last_ref[...] = result[:, lanes:]


def analyse(weights, pieces, rows, width):
    own = weights.shape[0]
    total = weights.shape[1]
    block = 128
    flat = [piece.reshape(piece.shape[0] * rows, width) for piece in pieces]
    out, first, last = pl.pallas_call(
        functools.partial(analysis_kernel, rows, len(flat)),
        grid=(width // block,),
        in_specs=[pl.BlockSpec((own, total), lambda i: (0, 0))]
        + [pl.BlockSpec((piece.shape[0], block), lambda i: (0, i)) for piece in flat],
        out_specs=[
            pl.BlockSpec((own * rows, block), lambda i: (0, i)),
            pl.BlockSpec((own, block), lambda i: (0, i)),
            pl.BlockSpec((own, block), lambda i: (0, i)),
        ],
        out_shape=[
            jax.ShapeDtypeStruct((own * rows, width), jnp.float32),
            jax.ShapeDtypeStruct((own, width), jnp.float32),
            jax.ShapeDtypeStruct((own, width), jnp.float32),
        ],
        name="analyse",
    )(weights, *flat)
    return out.reshape(own, rows, width), first, last


def sigmoid(value):
    return 0.5 + 0.5 * jnp.tanh(0.5 * value)


def step_kernel(edges, counts_ref, field, above, below, ksat, ksat_above, ksat_below, storage, recharge, out, *sides):
    rows, width = ksat.shape
    base = pl.program_id(0) * field.shape[0]
    line = lax.broadcasted_iota(jnp.int32, (rows, width), 0)
    column = lax.broadcasted_iota(jnp.int32, (rows, width), 1)

    def shifted(value, before, after):
        up = jnp.where(line == 0, before, pltpu.roll(value, 1, axis=0))
        down = jnp.where(line == rows - 1, after, pltpu.roll(value, rows - 1, axis=0))
        left = jnp.where(column == 0, 0.0, pltpu.roll(value, 1, axis=1))
        right = jnp.where(column == width - 1, 0.0, pltpu.roll(value, width - 1, axis=1))
        return up, down, left, right

    def one_member(member, carry):
        level = field[member]
        level_above = above[pl.ds(member, 1), :]
        level_below = below[pl.ds(member, 1), :]
        conduct = ksat[...] * sigmoid(level)
        conduct_above = ksat_above[...] * sigmoid(level_above)
        conduct_below = ksat_below[...] * sigmoid(level_below)
        flux = jnp.zeros_like(level)
        others = shifted(level, level_above, level_below)
        other_conducts = shifted(conduct, conduct_above, conduct_below)
        for other, other_conduct in zip(others, other_conducts):
            flux = flux + (conduct + other_conduct) * (other - level)
        goal = level + storage[...] * jnp.tanh(level) + (0.5 * flux + recharge[...])

        def sweep(index, iterate):
            held = storage[...]
            bend = jnp.tanh(iterate)
            slope = 1.0 + held * (1.0 - bend * bend)
            guess = pl.reciprocal(slope, approx=True)
            inverse = guess * (2.0 - slope * guess)
            return iterate - DAMPING * (iterate + held * bend - goal) * inverse

        result = lax.fori_loop(0, counts_ref[base + member], sweep, level)
        out[member] = result
        if edges:
            sides[0][pl.ds(member, 1), :] = result[:1]
            sides[1][pl.ds(member, 1), :] = result[rows - 1 :]
        return carry

    lax.fori_loop(0, field.shape[0], one_member, 0)


def forecast_step(field, above, below, ksat, ksat_above, ksat_below, storage, recharge, counts, edges):
    own, rows, width = field.shape
    cell_spec = pl.BlockSpec((rows, width), lambda i, c: (0, 0))
    line_spec = pl.BlockSpec((1, width), lambda i, c: (0, 0))
    side_spec = pl.BlockSpec((GROUP, width), lambda i, c: (i, 0))
    field_spec = pl.BlockSpec((GROUP, rows, width), lambda i, c: (i, 0, 0))
    side_shape = jax.ShapeDtypeStruct((own, width), jnp.float32)
    return pl.pallas_call(
        functools.partial(step_kernel, edges),
        grid_spec=pltpu.PrefetchScalarGridSpec(
            num_scalar_prefetch=1,
            grid=(own // GROUP,),
            in_specs=[field_spec, side_spec, side_spec, cell_spec, line_spec, line_spec, cell_spec, cell_spec],
            out_specs=[field_spec] + [side_spec] * (2 * edges),
        ),
        out_shape=[jax.ShapeDtypeStruct(field.shape, jnp.float32)] + [side_shape] * (2 * edges),
        name="forecast_step",
    )(counts, field, above, below, ksat, ksat_above, ksat_below, storage, recharge)


def from_neighbours(first, last):
    peers = lax.axis_size("space")
    upward = [(i, i + 1) for i in range(peers - 1)]
    downward = [(i + 1, i) for i in range(peers - 1)]
    return lax.ppermute(last, "space", upward), lax.ppermute(first, "space", downward)


def on_device(state, obs_index, obs_value, obs_scale, ksat, storage, recharge, newton_counts):
    local, rows, width = state.shape
    groups = lax.axis_size("member")
    devices = groups * lax.axis_size("space")
    members = local * groups
    position = lax.axis_index("member")
    root_count = jnp.sqrt(jnp.float32(members - 1))
    swap = [(i, i ^ 1) for i in range(groups)]

    pieces = [(state, position, 0), (lax.ppermute(state, "member", swap), position ^ 1, 0)]

    def send_chunk(source, low, high):
        for distance in range(2, groups, 2):
            route = [(i, (i + distance) % groups) for i in range(groups)]
            arrived = lax.ppermute(source[low:high], "member", route)
            pieces.append((arrived, (position + groups - distance) % groups, low))
            pieces.append((lax.ppermute(arrived, "member", swap), ((position ^ 1) + groups - distance) % groups, low))

    early = 8
    send_chunk(state, 0, early)

    local_obs = jnp.take(state.reshape(local, rows * width), obs_index, axis=1)
    sampled = lax.all_to_all(local_obs, "member", split_axis=1, concat_axis=0, tiled=True)
    part = obs_index.shape[0] // groups
    scale = lax.dynamic_slice_in_dim(obs_scale, position * part, part)
    value = lax.dynamic_slice_in_dim(obs_value, position * part, part)
    mean_obs = jnp.mean(sampled, axis=0)
    spread = (sampled - mean_obs) * scale / root_count
    innovation = scale * (value - mean_obs)
    right = jnp.concatenate([spread, innovation[None], jnp.zeros((127, part), jnp.float32)], axis=0)
    partial = jnp.dot(spread, right.T, precision=HIGHEST_PRECISION)
    partial = partial.reshape(devices, members // devices, members + 128)
    partial = lax.all_to_all(partial, ("member", "space"), split_axis=0, concat_axis=0)
    summed = lax.all_gather(jnp.sum(partial, axis=0), ("member", "space"), axis=0, tiled=True)
    late_state, summed = lax.optimization_barrier((state, summed))

    middle = (early + local) // 2 // 8 * 8
    send_chunk(late_state, early, middle)
    send_chunk(late_state, middle, local)

    drive_vector = summed[:, members]
    root_inverse = inverse_root(summed[:, :members])
    mean_weights = jnp.dot(
        root_inverse,
        jnp.dot(root_inverse, drive_vector, precision=HIGHEST_PRECISION),
        precision=HIGHEST_PRECISION,
    )
    transform = mean_weights[:, None] / root_count + root_inverse
    own_columns = lax.dynamic_slice_in_dim(transform, position * local, local, axis=1)
    weights = (own_columns - jnp.mean(own_columns, axis=0) + 1.0 / members).T
    ordered = jnp.concatenate(
        [
            lax.dynamic_slice_in_dim(weights, source * local + low, piece.shape[0], axis=1)
            for piece, source, low in pieces
        ],
        axis=1,
    )
    field, first, last = analyse(ordered, [piece for piece, source, low in pieces], rows, width)

    counts = lax.dynamic_slice_in_dim(newton_counts, position * local, local)
    ksat_above, ksat_below = from_neighbours(ksat[:1], ksat[rows - 1 :])
    above, below = from_neighbours(first, last)
    field, first, last = forecast_step(
        field, above, below, ksat, ksat_above, ksat_below, storage, recharge, counts, True
    )
    above, below = from_neighbours(first, last)
    (field,) = forecast_step(
        field, above, below, ksat, ksat_above, ksat_below, storage, recharge, counts, False
    )
    return field


def solution(mesh):
    return jax.shard_map(
        on_device,
        mesh=mesh,
        in_specs=(
            P("member", "space", None),
            P("space"),
            P("space"),
            P("space"),
            P("space", None),
            P("space", None),
            P("space", None),
            P(),
        ),
        out_specs=P("member", "space", None),
        check_vma=False,
    )
```
